8 devices in a mesh: rep: 2 (over y, z), dp: 4 (over x, core).
Axes of the slice: x: 2, y: 2, z: 1, core: 2. Of those that a mesh axis runs over, the one named last changes fastest.
Arguments:
- x: bfloat16 [8, 2048, 512], P(('rep', 'dp')), parts along dimension 0
- dy: bfloat16 [8, 2048, 512], P(('rep', 'dp')), parts along dimension 0
- w_gate: bfloat16 [2, 512, 4096], P(None, 'dp')
- w_up: bfloat16 [2, 512, 4096], P(None, 'dp')
- w_down: bfloat16 [2, 4096, 512], P(None, 'dp')
- m_w_gate: float32 [2, 512, 4096], P(None, 'dp')
- m_w_up: float32 [2, 512, 4096], P(None, 'dp')
- m_w_down: float32 [2, 4096, 512], P(None, 'dp')
- v_w_gate: float32 [2, 512, 4096], P(None, 'dp')
- v_w_up: float32 [2, 512, 4096], P(None, 'dp')
- v_w_down: float32 [2, 4096, 512], P(None, 'dp')
Outputs:
- output 1: bfloat16 [4, 512, 4096], P('rep', 'dp'), parts along dimension 0
- output 2: bfloat16 [4, 512, 4096], P('rep', 'dp'), parts along dimension 0
- output 3: bfloat16 [4, 4096, 512], P('rep', 'dp'), parts along dimension 0
- output 4: float32 [4, 512, 4096], P('rep', 'dp'), parts along dimension 0
- output 5: float32 [4, 512, 4096], P('rep', 'dp'), parts along dimension 0
- output 6: float32 [4, 4096, 512], P('rep', 'dp'), parts along dimension 0
- output 7: float32 [4, 512, 4096], P('rep', 'dp'), parts along dimension 0
- output 8: float32 [4, 512, 4096], P('rep', 'dp'), parts along dimension 0
- output 9: float32 [4, 4096, 512], P('rep', 'dp'), parts along dimension 0
There are 2 independent parts. The reference program is written for one: setup_inputs(seed, part) draws one part's arguments, and reference() takes and returns one part's arrays. A program takes and returns all parts, laid end to end along the dimension named above; an argument that names none is the same for every part.
All inputs are finite; a program needn't handle non-finite values.
Results may differ from the reference program's by a relative error of at most 0.022.
Values are sent between devices in bfloat16 or wider.
A program may use at most 2 GiB of HBM per device.

```python
import jax
import jax.numpy as jnp
from jax import lax

SEQUENCES = 4
TOKENS = 2048
D = 512
FF = 4096
LAYERS = 2
NAMES = ("w_gate", "w_up", "w_down")
SHAPES = {"w_gate": (LAYERS, D, FF), "w_up": (LAYERS, D, FF), "w_down": (LAYERS, FF, D)}


def bump(key, n, height):
    away = (jnp.arange(n, dtype=jnp.int32) - jax.random.randint(key, (), 0, n, jnp.int32)) % n
    return jnp.where(away < n // 8, height, 1.0)


def together(key, own, strength):
    shared = jax.random.normal(key, own.shape[1:], jnp.float32)
    return (own + strength * shared) * lax.rsqrt(1 + strength * strength)


def setup_inputs(seed: int = 0, part: int = 0) -> dict:
    kx, kdy, ka, kb, kz, kf, kh, kl, *keys = jax.random.split(jax.random.key(seed), 8 + 3 * len(NAMES))
    kx, kdy, ka, kb = (jax.random.fold_in(k, part) for k in (kx, kdy, ka, kb))
    kw, km, kv = (keys[i::3] for i in range(3))
    shape = (SEQUENCES, TOKENS, D)
    much_x, much_dy = jax.random.uniform(kz, (2,), jnp.float32, 0.0, 1.0)
    loud = 2.0 ** jax.random.uniform(jax.random.fold_in(kz, 1), (), jnp.float32, -1.0, 2.0)
    layers = 2.0 ** jax.random.uniform(kl, (LAYERS, 1, 1), jnp.float32, -1.0, 1.0)
    x = together(ka, jax.random.normal(kx, shape, jnp.float32), much_x) * bump(kf, D, 4.0)
    dy = together(kb, jax.random.normal(kdy, shape, jnp.float32), much_dy)
    drawn = {"x": x.astype(jnp.bfloat16), "dy": (loud * dy * (SEQUENCES * TOKENS) ** -0.5).astype(jnp.bfloat16)}
    for key, name in zip(kw, NAMES, strict=True):
        w = jax.random.normal(key, SHAPES[name], jnp.float32) * SHAPES[name][1] ** -0.5
        drawn[name] = (w * {"w_gate": 1.0, "w_up": bump(kh, FF, 4.0), "w_down": layers}[name]).astype(jnp.bfloat16)
    for key, name in zip(km, NAMES, strict=True):
        drawn[f"m_{name}"] = 0.1 * jax.random.normal(key, SHAPES[name], jnp.float32)
    for key, name in zip(kv, NAMES, strict=True):
        drawn[f"v_{name}"] = jax.random.uniform(key, SHAPES[name], jnp.float32, 0.005, 0.015)
    return drawn


def matmul(a, w):
    return jnp.dot(a, w, preferred_element_type=jnp.float32).astype(jnp.bfloat16)


def normed(h):
    wide = h.astype(jnp.float32)
    scale = lax.rsqrt(jnp.mean(wide**2, -1, keepdims=True) + 1e-6)
    return (wide * scale).astype(jnp.bfloat16)


def layer(h, w):
    a = normed(h)
    gate = jnp.dot(a, w["w_gate"], preferred_element_type=jnp.float32)
    up = jnp.dot(a, w["w_up"], preferred_element_type=jnp.float32)
    return h + matmul((jax.nn.silu(gate) * up).astype(jnp.bfloat16), w["w_down"])


def adamw(w, m, v, g):
    m = 0.9 * m + 0.1 * g
    v = 0.95 * v + 0.05 * g * g
    step = m * lax.rsqrt(v + 1e-8) + 0.1 * w
    return (w - 0.02 * step).astype(jnp.bfloat16), m, v


def clipped(gradients, sum_of_squares, count):
    factor = jnp.minimum(1.0, 0.5 * lax.rsqrt(sum_of_squares / count + 1e-30))
    return [g * factor for g in gradients]


def stack(weights, h):
    return lax.scan(lambda h, w: (layer(h, w), None), h, weights)[0]


def reference(x, dy, w_gate, w_up, w_down, m_w_gate, m_w_up, m_w_down, v_w_gate, v_w_up, v_w_down):
    weights = dict(zip(NAMES, (w_gate, w_up, w_down), strict=True))

    def take(so_far, sequence):
        h, by_y = sequence
        _, back = jax.vjp(lambda w: stack(w, h), weights)
        return jax.tree.map(lambda total, term: total + term.astype(jnp.float32), so_far, back(by_y)[0]), None

    none_yet = {name: jnp.zeros(w.shape, jnp.float32) for name, w in weights.items()}
    by_weights, _ = lax.scan(take, none_yet, (x, dy))
    gradients = [by_weights[name].astype(jnp.bfloat16).astype(jnp.float32) for name in NAMES]
    gradients = clipped(gradients, sum(jnp.sum(g * g) for g in gradients), sum(g.size for g in gradients))
    new = [
        adamw(w.astype(jnp.float32), m, v, g)
        for w, m, v, g in zip((w_gate, w_up, w_down), (m_w_gate, m_w_up, m_w_down), (v_w_gate, v_w_up, v_w_down), gradients, strict=True)
    ]
    return tuple(one[which] for which in range(3) for one in new)
```

```python
import functools

import jax
import jax.numpy as jnp
from jax import lax
from jax.experimental import pallas as pl
from jax.experimental.pallas import tpu as pltpu
from jax.sharding import PartitionSpec as P

MESH = pl.DeviceIdType.MESH
F32, BF16 = jnp.float32, jnp.bfloat16
T, D, FF = 2048, 512, 4096
CH = 8
B = 128
C = 4 * B
TT = 512
N = 2 * CH


def dot(a, b):
    return jnp.dot(a, b, preferred_element_type=F32)


def dot_nt(a, b):
    return lax.dot_general(a, b, (((1,), (1,)), ((), ())), preferred_element_type=F32)


def normed(h):
    wide = h.astype(F32)
    return (wide * lax.rsqrt(jnp.mean(wide * wide, -1, keepdims=True) + 1e-6)).astype(BF16)


def kernel(
    x_ref, dy_ref, wg_ref, wu_ref, wd_ref, gg_ref, gu_ref, gd_ref, sq_ref,
    W, A, H, AT, DY, DYT, ACC, PB, DG, DU, G, R, X, XR, SO, GB, SQ,
    own_s, xs, xr, ys, yr, ds, dr, es, er, rs, rr, zs, zr, ld, gs, credit,
):
    me, rep = lax.axis_index("dp"), lax.axis_index("rep")
    core, chip = lax.rem(me, 2), lax.div(me, 2)
    xp, mate = lax.rem(me + 2, 4), me + 1 - 2 * core
    matexp = lax.rem(mate + 2, 4)
    to_x, to_mate, to_y = {"dp": xp}, {"dp": mate}, {"rep": 1 - rep}
    half = pl.ds(pl.multiple_of(64 * rep, 64), 64)
    other_half = pl.ds(pl.multiple_of(64 * (1 - rep), 64), 64)

    barrier = pltpu.get_barrier_semaphore()
    for to in (to_x, to_mate, to_y):
        pl.semaphore_signal(barrier, inc=1, device_id=to, device_id_type=MESH)

    def split(n):
        return lax.div(n, CH), lax.rem(n, CH)

    def own(n, _):
        l, i = split(n)
        for d in range(4):
            cols = pl.ds(pl.multiple_of(1024 * d + B * i, B), B)
            pltpu.make_async_copy(wg_ref.at[l, :, cols], W.at[l, i, me, 0, :, pl.ds(B * d, B)], own_s.at[n]).start()
            pltpu.make_async_copy(wu_ref.at[l, :, cols], W.at[l, i, me, 1, :, pl.ds(B * d, B)], own_s.at[n]).start()
        pltpu.make_async_copy(wd_ref.at[l, pl.ds(pl.multiple_of(B * i, B), B), :], W.at[l, i, me, 2], own_s.at[n]).start()
        return 0

    lax.fori_loop(0, CH, own, 0)
    pltpu.make_async_copy(x_ref, A, ld.at[0]).start()
    pltpu.make_async_copy(dy_ref, DY, ld.at[1]).start()
    pltpu.make_async_copy(x_ref, H, ld.at[2]).start()
    lax.fori_loop(CH, N, own, 0)

    def remote(src, dst, s, r, to):
        return pltpu.make_async_remote_copy(src_ref=src, dst_ref=dst, send_sem=s, recv_sem=r, device_id=to, device_id_type=MESH)

    def move_x(n, block=None):
        l, i = split(n)
        ref = W.at[l, i, me if block is None else block, :, half, :]
        return remote(ref, ref, xs.at[n], xr.at[n], to_x)

    def move_y(n, which):
        l, i = split(n)
        ref = W.at[l, i, xp, :, which, :]
        return remote(ref, ref, ys.at[n], yr.at[n], to_y)

    def move_d(n, block):
        l, i = split(n)
        ref = W.at[l, i, block]
        return remote(ref, ref, ds.at[n], dr.at[n], to_mate)

    def move_e(n, block):
        l, i = split(n)
        ref = W.at[l, i, block]
        return remote(ref, ref, es.at[n], er.at[n], to_mate)

    pl.semaphore_wait(barrier, 3)

    def send_own(n, _):
        l, i = split(n)
        pltpu.make_async_copy(W.at[l, i, me], W.at[l, i, me], own_s.at[n]).wait()
        move_x(n).start()
        move_d(n, me).start()
        return 0

    lax.fori_loop(0, N, send_own, 0)

    def pump_x(n):
        move_x(n, xp).wait_recv()
        move_y(n, half).start()

    def pump_y(n):
        move_y(n, other_half).wait_recv()
        move_e(n, xp).start()

    def arrive(n):
        @pl.when(n + 2 < N)
        def _():
            pump_x(n + 2)

        @pl.when(n + 1 < N)
        def _():
            pump_y(n + 1)

        move_d(n, mate).wait_recv()
        move_e(n, matexp).wait_recv()

    def tiles(body):
        def one(t, _):
            body(pl.ds(pl.multiple_of(t * TT, TT), TT))
            return 0

        lax.fori_loop(0, T // TT, one, 0)

    def columns(t):
        return pl.ds(pl.multiple_of(t * TT, TT), TT)

    def transposed(src, dst):
        def one(t, _):
            dst[:, columns(t)] = src[columns(t), :].T
            return 0

        lax.fori_loop(0, T // TT, one, 0)

    pltpu.make_async_copy(x_ref, A, ld.at[0]).wait()

    def norm_a(rows):
        A[rows, :] = normed(A[rows, :])
        ACC[rows, :] = jnp.zeros((TT, D), F32)

    tiles(norm_a)
    pltpu.make_async_copy(dy_ref, DY, ld.at[1]).wait()
    transposed(DY, DYT)
    pltpu.make_async_copy(x_ref, H, ld.at[2]).wait()
    SQ[...] = jnp.zeros_like(SQ)

    pump_x(0)
    pump_x(1)
    pump_y(0)

    def matrix(l, i, which):
        return W[l, i, :, which].reshape(4 * B, 512)

    def forward(i, _):
        arrive(i)

        def tile(rows):
            a = A[rows, :]
            gate, up = dot(a, matrix(0, i, 0)), dot(a, matrix(0, i, 1))
            p = (gate * jax.nn.sigmoid(gate) * up).astype(BF16)
            ACC[rows, :] += dot(p, matrix(0, i, 2))

        tiles(tile)
        return 0

    lax.fori_loop(0, CH, forward, 0)

    def between(rows):
        h = (H[rows, :].astype(F32) + ACC[rows, :].astype(BF16).astype(F32)).astype(BF16)
        H[rows, :] = h
        A[rows, :] = normed(h)
        ACC[rows, :] = jnp.zeros((TT, D), F32)

    tiles(between)
    transposed(A, AT)

    def to_core(q):
        return remote(G.at[lax.rem(q, 2), 1 - core], R.at[lax.rem(q, 2)], rs.at[q], rr.at[q], to_mate)

    def to_chip(q):
        return remote(X.at[lax.rem(q, 3)], XR.at[lax.rem(q, 6)], zs.at[q], zr.at[q], to_x)

    def on_chip(q):
        slot = lax.rem(q, 2)
        to_core(q).wait_recv()

        @pl.when(q >= 3)
        def _():
            to_chip(q - 3).wait_send()

        for j in range(3):
            X[lax.rem(q, 3), j] = (G[slot, core, 1 - chip, j].astype(F32) + R[slot, 1 - chip, j].astype(F32)).astype(BF16)
            SO[lax.rem(q, 3), j] = G[slot, core, chip, j].astype(F32) + R[slot, chip, j].astype(F32)

        @pl.when(q >= 6)
        def _():
            pl.semaphore_wait(credit, 1)

        to_chip(q).start()

    def put(q, slot):
        l, i = 1 - lax.div(q, CH), lax.rem(q, CH)
        for d in range(4):
            cols = pl.ds(pl.multiple_of(1024 * d + B * i, B), B)
            pltpu.make_async_copy(GB.at[slot, 0, :, pl.ds(B * d, B)], gg_ref.at[l, :, cols], gs.at[slot]).start()
            pltpu.make_async_copy(GB.at[slot, 1, :, pl.ds(B * d, B)], gu_ref.at[l, :, cols], gs.at[slot]).start()
        pltpu.make_async_copy(GB.at[slot, 2], gd_ref.at[l, pl.ds(pl.multiple_of(B * i, B), B), :], gs.at[slot]).start()

    def put_wait(slot):
        pltpu.make_async_copy(GB.at[slot], GB.at[slot], gs.at[slot]).wait()

    def final(q):
        slot = lax.rem(q, 2)
        to_chip(q).wait_recv()

        @pl.when(q >= 2)
        def _():
            put_wait(slot)

        for j in range(3):
            g = (SO[lax.rem(q, 3), j] + XR[lax.rem(q, 6), j].astype(F32)).astype(BF16)
            GB[slot, j] = g
            wide = g.astype(F32)
            SQ[...] += jnp.sum((wide * wide).reshape(B // 8, 8, 512), axis=0)

        @pl.when(q < N - 6)
        def _():
            pl.semaphore_signal(credit, inc=1, device_id=to_x, device_id_type=MESH)

        put(q, slot)

    def backward(q, i, l):
        def tile(rows):
            a, by = A[rows, :], DY[rows, :]
            wg, wu = matrix(l, i, 0), matrix(l, i, 1)
            gate, up = dot(a, wg), dot(a, wu)
            dp = dot_nt(by, matrix(l, i, 2)).astype(BF16).astype(F32)
            s = jax.nn.sigmoid(gate)
            silu = gate * s
            PB[rows, :] = (silu * up).astype(BF16)
            du = (dp * silu).astype(BF16)
            dg = (dp * up * (s + silu * (1.0 - s))).astype(BF16)
            DU[rows, :] = du
            DG[rows, :] = dg
            if l == 1:
                ACC[rows, :] += dot_nt(dg, wg) + dot_nt(du, wu)

        tiles(tile)

        @pl.when(q >= 4)
        def _():
            final(q - 4)

        @pl.when(q >= 1)
        def _():
            on_chip(q - 1)

        @pl.when(q >= 2)
        def _():
            to_core(q - 2).wait_send()

        slot = lax.rem(q, 2)
        for j, made in enumerate((lambda: dot(AT[...], DG[...]), lambda: dot(AT[...], DU[...]), lambda: dot(DYT[...], PB[...]).T)):
            by_w = made().astype(BF16)
            for d in range(4):
                G[slot, d % 2, d // 2, j] = by_w[B * d : B * (d + 1)]
        to_core(q).start()

    def last_layer(i, _):
        arrive(CH + i)
        backward(i, i, 1)
        return 0

    lax.fori_loop(0, CH, last_layer, 0)

    again = pltpu.make_async_copy(x_ref, A, ld.at[0])
    again.start()

    def norm_back(rows):
        h, da = H[rows, :].astype(F32), ACC[rows, :].astype(BF16).astype(F32)
        scale = lax.rsqrt(jnp.mean(h * h, -1, keepdims=True) + 1e-6)
        inner = jnp.sum(da * h, -1, keepdims=True)
        by_h = da * scale - h * (inner * scale * scale * scale * (1.0 / D))
        DY[rows, :] = (DY[rows, :].astype(F32) + by_h.astype(BF16).astype(F32)).astype(BF16)

    tiles(norm_back)
    transposed(DY, DYT)
    again.wait()

    def norm_again(rows):
        A[rows, :] = normed(A[rows, :])

    tiles(norm_again)
    transposed(A, AT)

    def first_layer(i, _):
        backward(CH + i, i, 0)
        return 0

    lax.fori_loop(0, CH, first_layer, 0)

    final(N - 4)
    on_chip(N - 1)
    for q in range(N - 3, N):
        final(q)
    sq_ref[...] = SQ[...]
    put_wait(0)
    put_wait(1)

    def drain(n, _):
        move_x(n).wait_send()
        move_y(n, half).wait_send()
        move_d(n, me).wait_send()
        move_e(n, xp).wait_send()
        return 0

    lax.fori_loop(0, N, drain, 0)
    for q in range(N - 2, N):
        to_core(q).wait_send()
    for q in range(N - 3, N):
        to_chip(q).wait_send()


def gradients(x, dy, wg, wu, wd):
    any_space, vmem = pl.BlockSpec(memory_space=pl.ANY), pl.BlockSpec(memory_space=pltpu.VMEM)
    sems = [pltpu.SemaphoreType.DMA((N,))] * 13 + [pltpu.SemaphoreType.DMA((3,)), pltpu.SemaphoreType.DMA((2,)), pltpu.SemaphoreType.REGULAR]
    block = (3, B, 512)
    return pl.pallas_call(
        kernel,
        out_shape=(
            jax.ShapeDtypeStruct(wg.shape, BF16),
            jax.ShapeDtypeStruct(wu.shape, BF16),
            jax.ShapeDtypeStruct(wd.shape, BF16),
            jax.ShapeDtypeStruct((8, 512), F32),
        ),
        in_specs=[any_space] * 5,
        out_specs=(any_space, any_space, any_space, vmem),
        scratch_shapes=[
            pltpu.VMEM((2, CH, 4) + block, BF16),
            pltpu.VMEM((T, D), BF16),
            pltpu.VMEM((T, D), BF16),
            pltpu.VMEM((D, T), BF16),
            pltpu.VMEM((T, D), BF16),
            pltpu.VMEM((D, T), BF16),
            pltpu.VMEM((T, D), F32),
            pltpu.VMEM((T, C), BF16),
            pltpu.VMEM((T, C), BF16),
            pltpu.VMEM((T, C), BF16),
            pltpu.VMEM((2, 2, 2) + block, BF16),
            pltpu.VMEM((2, 2) + block, BF16),
            pltpu.VMEM((3,) + block, BF16),
            pltpu.VMEM((6,) + block, BF16),
            pltpu.VMEM((3,) + block, F32),
            pltpu.VMEM((2,) + block, BF16),
            pltpu.VMEM((8, 512), F32),
        ]
        + sems,
        compiler_params=pltpu.CompilerParams(collective_id=0, has_side_effects=True, vmem_limit_bytes=67043328),
        name="step",
    )(x, dy, wg, wu, wd)


def adamw(w, m, v, g):
    m = 0.9 * m + 0.1 * g
    v = 0.95 * v + 0.05 * g * g
    step = m * lax.rsqrt(v + 1e-8) + 0.1 * w
    return (w - 0.02 * step).astype(BF16), m, v


def solution(mesh):
    def step(x, dy, *arrays):
        weights, m, v = (arrays[i : i + 3] for i in (0, 3, 6))
        *grads, squares = gradients(x[0], dy[0], *weights)
        total = lax.psum(jnp.sum(squares), "dp")
        count = 4 * sum(g.size for g in grads)
        factor = jnp.minimum(1.0, 0.5 * lax.rsqrt(total / count + 1e-30))
        new = [adamw(w.astype(F32), m, v, g.astype(F32) * factor) for w, m, v, g in zip(weights, m, v, grads, strict=True)]
        return tuple(one[which] for which in range(3) for one in new)

    states, cut = P(("rep", "dp"), None, None), P(None, "dp", None)
    return jax.shard_map(
        step,
        mesh=mesh,
        in_specs=(states, states) + (cut,) * 9,
        out_specs=(P("rep", "dp", None),) * 9,
        check_vma=False,
    )
```

```python
import functools

import jax
import jax.numpy as jnp
from jax import lax
from jax.experimental import pallas as pl
from jax.experimental.pallas import tpu as pltpu
from jax.sharding import PartitionSpec as P

MESH = pl.DeviceIdType.MESH
F32, BF16 = jnp.float32, jnp.bfloat16
T, D, FF = 2048, 512, 4096
CH = 8
B = 128
C = 4 * B
TT = 512
N = 2 * CH


def dot(a, b):
    return jnp.dot(a, b, preferred_element_type=F32)


def dot_nt(a, b):
    return lax.dot_general(a, b, (((1,), (1,)), ((), ())), preferred_element_type=F32)


def normed(h):
    wide = h.astype(F32)
    return (wide * lax.rsqrt(jnp.mean(wide * wide, -1, keepdims=True) + 1e-6)).astype(BF16)


def kernel(
    x_ref, dy_ref, wg_ref, wu_ref, wd_ref, gg_ref, gu_ref, gd_ref, sq_ref,
    W, A0, A0T, A1, A1T, H, DY, DYT, ACC, PB0, PB1, DG0, DG1, DU0, DU1, AW, G, R, X, XR, SO, GB, SQ, S, SR,
    xs, xr, ys, yr, es, er, own_s, ds, dr, rs, rr, zs, zr, ld, gs, ss, sr, credit,
):
    me, rep = lax.axis_index("dp"), lax.axis_index("rep")
    core, chip = lax.rem(me, 2), lax.div(me, 2)
    xp, mate = lax.rem(me + 2, 4), me + 1 - 2 * core
    matexp = lax.rem(mate + 2, 4)
    to_x, to_mate, to_y = {"dp": xp}, {"dp": mate}, {"rep": 1 - rep}
    half = pl.ds(pl.multiple_of(64 * rep, 64), 64)
    other_half = pl.ds(pl.multiple_of(64 * (1 - rep), 64), 64)

    barrier = pltpu.get_barrier_semaphore()
    for to in (to_x, to_mate, to_y):
        pl.semaphore_signal(barrier, inc=1, device_id=to, device_id_type=MESH)

    def split(n):
        return lax.div(n, CH), lax.rem(n, CH)

    def own(n, _):
        l, i = split(n)
        for d in range(4):
            cols = pl.ds(pl.multiple_of(1024 * d + B * i, B), B)
            pltpu.make_async_copy(wg_ref.at[l, :, cols], W.at[l, i, me, 0, :, pl.ds(B * d, B)], own_s.at[n]).start()
            pltpu.make_async_copy(wu_ref.at[l, :, cols], W.at[l, i, me, 1, :, pl.ds(B * d, B)], own_s.at[n]).start()
        pltpu.make_async_copy(wd_ref.at[l, pl.ds(pl.multiple_of(B * i, B), B), :], W.at[l, i, me, 2], own_s.at[n]).start()
        return 0

    lax.fori_loop(0, CH, own, 0)
    pltpu.make_async_copy(x_ref, A0, ld.at[0]).start()
    pltpu.make_async_copy(dy_ref, DY, ld.at[1]).start()
    pltpu.make_async_copy(x_ref, H, ld.at[2]).start()
    lax.fori_loop(CH, N, own, 0)

    def remote(src, dst, s, r, to):
        return pltpu.make_async_remote_copy(src_ref=src, dst_ref=dst, send_sem=s, recv_sem=r, device_id=to, device_id_type=MESH)

    def piece(u):
        n = lax.div(u, 3)
        return split(n) + (lax.rem(u, 3),)

    def move_x(u, block=None):
        l, i, j = piece(u)
        ref = W.at[l, i, me if block is None else block, j, half, :]
        return remote(ref, ref, xs.at[u], xr.at[u], to_x)

    def move_y(u, which):
        l, i, j = piece(u)
        ref = W.at[l, i, xp, j, which, :]
        return remote(ref, ref, ys.at[u], yr.at[u], to_y)

    def move_e(u, block):
        l, i, j = piece(u)
        ref = W.at[l, i, block, j]
        return remote(ref, ref, es.at[u], er.at[u], to_mate)

    def move_d(n, block):
        l, i = split(n)
        ref = W.at[l, i, block]
        return remote(ref, ref, ds.at[n], dr.at[n], to_mate)

    pl.semaphore_wait(barrier, 3)

    def send_own(n, _):
        l, i = split(n)
        pltpu.make_async_copy(W.at[l, i, me], W.at[l, i, me], own_s.at[n]).wait()
        for j in range(3):
            move_x(3 * n + j).start()
        move_d(n, me).start()
        return 0

    lax.fori_loop(0, N, send_own, 0)

    def pump_x(u):
        move_x(u, xp).wait_recv()
        move_y(u, half).start()

    def pump_y(u):
        move_y(u, other_half).wait_recv()
        move_e(u, xp).start()

    def arrive(n):
        move_d(n, mate).wait_recv()
        for j in range(3):
            move_e(3 * n + j, matexp).wait_recv()

    def tiles(body):
        def one(t, _):
            body(pl.ds(pl.multiple_of(t * TT, TT), TT))
            return 0

        lax.fori_loop(0, T // TT, one, 0)

    def columns(t):
        return pl.ds(pl.multiple_of(t * TT, TT), TT)

    def transposed(src, dst):
        def one(t, _):
            dst[:, columns(t)] = src[columns(t), :].T
            return 0

        lax.fori_loop(0, T // TT, one, 0)

    pltpu.make_async_copy(x_ref, A0, ld.at[0]).wait()

    def norm_a(rows):
        A0[rows, :] = normed(A0[rows, :])
        ACC[rows, :] = jnp.zeros((TT, D), F32)

    tiles(norm_a)
    pump_x(0)
    pump_x(1)
    pltpu.make_async_copy(dy_ref, DY, ld.at[1]).wait()
    transposed(DY, DYT)
    pump_x(2)
    pump_y(0)
    pltpu.make_async_copy(x_ref, H, ld.at[2]).wait()
    transposed(A0, A0T)
    SQ[...] = jnp.zeros_like(SQ)
    pump_x(3)
    pump_y(1)
    pump_x(4)
    pump_y(2)

    def matrix(l, i, which):
        return W[l, i, :, which].reshape(4 * B, 512)

    def forward(i, _):
        arrive(i)
        for t in range(T // TT):
            if t > 0:
                pump_x(3 * i + t + 4)
                pump_y(3 * i + t + 2)
            rows = slice(t * TT, (t + 1) * TT)
            a = A0[rows, :]
            gate, up = dot(a, matrix(0, i, 0)), dot(a, matrix(0, i, 1))
            p = (gate * jax.nn.sigmoid(gate) * up).astype(BF16)
            ACC[rows, :] += dot(p, matrix(0, i, 2))
        return 0

    lax.fori_loop(0, CH, forward, 0)

    def between(rows):
        h = (H[rows, :].astype(F32) + ACC[rows, :].astype(BF16).astype(F32)).astype(BF16)
        H[rows, :] = h
        A1[rows, :] = normed(h)
        ACC[rows, :] = jnp.zeros((TT, D), F32)

    tiles(between)
    transposed(A1, A1T)

    def to_core(q):
        return remote(G.at[lax.rem(q, 2), 1 - core], R.at[lax.rem(q, 2)], rs.at[q], rr.at[q], to_mate)

    def to_chip(q):
        return remote(X.at[lax.rem(q, 3)], XR.at[lax.rem(q, 6)], zs.at[q], zr.at[q], to_x)

    def on_chip(q):
        slot = lax.rem(q, 2)
        to_core(q).wait_recv()

        @pl.when(q >= 3)
        def _():
            to_chip(q - 3).wait_send()

        for j in range(3):
            X[lax.rem(q, 3), j] = (G[slot, core, 1 - chip, j].astype(F32) + R[slot, 1 - chip, j].astype(F32)).astype(BF16)
            SO[lax.rem(q, 4), j] = G[slot, core, chip, j].astype(F32) + R[slot, chip, j].astype(F32)

        @pl.when(q >= 6)
        def _():
            pl.semaphore_wait(credit, 1)

        to_chip(q).start()

    def put(q, slot):
        l, i = 1 - lax.div(q, CH), lax.rem(q, CH)
        for d in range(4):
            cols = pl.ds(pl.multiple_of(1024 * d + B * i, B), B)
            pltpu.make_async_copy(GB.at[slot, 0, :, pl.ds(B * d, B)], gg_ref.at[l, :, cols], gs.at[slot]).start()
            pltpu.make_async_copy(GB.at[slot, 1, :, pl.ds(B * d, B)], gu_ref.at[l, :, cols], gs.at[slot]).start()
        pltpu.make_async_copy(GB.at[slot, 2], gd_ref.at[l, pl.ds(pl.multiple_of(B * i, B), B), :], gs.at[slot]).start()

    def put_wait(slot):
        pltpu.make_async_copy(GB.at[slot], GB.at[slot], gs.at[slot]).wait()

    def final(q):
        slot = lax.rem(q, 2)
        to_chip(q).wait_recv()

        @pl.when(q >= 2)
        def _():
            put_wait(slot)

        for j in range(3):
            g = (SO[lax.rem(q, 4), j] + XR[lax.rem(q, 6), j].astype(F32)).astype(BF16)
            GB[slot, j] = g
            wide = g.astype(F32)
            SQ[...] += jnp.sum((wide * wide).reshape(B // 8, 8, 512), axis=0)

        @pl.when(q < N - 6)
        def _():
            pl.semaphore_signal(credit, inc=1, device_id=to_x, device_id_type=MESH)

        put(q, slot)

    PB, DG, DU = (PB0, PB1), (DG0, DG1), (DU0, DU1)

    def tokens(n):
        return pl.ds(pl.multiple_of(lax.rem(n, 4) * TT, TT), TT)

    def first_half(n, slot, l, h):
        i, rows, cols = lax.div(n, 4), tokens(n), slice(256 * h, 256 * (h + 1))
        a, by = (A0, A1)[l][rows, :], DY[rows, :]
        gate = dot(a, W[l, i, :, 0, :, cols].reshape(D, 256))
        up = dot(a, W[l, i, :, 1, :, cols].reshape(D, 256))
        dp = dot_nt(by, W[l, i, 2 * h : 2 * h + 2, 2].reshape(256, D)).astype(BF16).astype(F32)
        s = jax.nn.sigmoid(gate)
        silu = gate * s
        PB[slot][:, cols] = (silu * up).astype(BF16)
        DU[slot][:, cols] = (dp * silu).astype(BF16)
        DG[slot][:, cols] = (dp * up * (s + silu * (1.0 - s))).astype(BF16)

    def by_input(n, slot, l):
        if l == 1:
            i, rows = lax.div(n, 4), tokens(n)
            ACC[rows, :] += dot_nt(DG[slot][...], matrix(l, i, 0)) + dot_nt(DU[slot][...], matrix(l, i, 1))

    def by_weight(n, slot, l, j):
        left = (A0T, A1T)[l] if j < 2 else DYT
        right = (DG, DU, PB)[j][slot]
        new = dot(left[:, tokens(n)], right[...])
        AW[j] = jnp.where(lax.rem(n, 4) == 0, 0.0, AW[j]) + new

    def both(n, slot, l):
        first_half(n + 1, 1 - slot, l, 0)
        by_input(n, slot, l)
        if l == 0:
            by_weight(n, slot, l, 0)
        first_half(n + 1, 1 - slot, l, 1)
        for j in range(1 - l, 3):
            by_weight(n, slot, l, j)

    def second(n, slot, l):
        by_input(n, slot, l)
        for j in range(3):
            by_weight(n, slot, l, j)

    def emit(q):
        @pl.when(q >= 2)
        def _():
            to_core(q - 2).wait_send()

        slot = lax.rem(q, 2)
        for j in range(3):
            by_w = AW[j].T.astype(BF16) if j == 2 else AW[j].astype(BF16)
            for d in range(4):
                G[slot, d % 2, d // 2, j] = by_w[B * d : B * (d + 1)]
        to_core(q).start()

    def sums(q):
        @pl.when(q >= 4)
        def _():
            final(q - 4)

        @pl.when((q >= 1) & (q != CH) & (q != CH + 1))
        def _():
            on_chip(q - 1)

    PAIRS = 2 * CH

    def layer_back(l):
        q0 = CH * (1 - l)

        def pair(j, _):
            i = lax.div(j, 2)
            if l == 1:
                for k in range(3):

                    @pl.when((26 + 3 * j + k >= 27) & (26 + 3 * j + k < 3 * N))
                    def _():
                        pump_y(26 + 3 * j + k)

                for k in range(3):

                    @pl.when(29 + 3 * j + k < 3 * N)
                    def _():
                        pump_x(29 + 3 * j + k)

                @pl.when(lax.rem(j, 2) == 1)
                def _():
                    arrive(CH + i + 1)

            both(2 * j, 0, l)
            both(2 * j + 1, 1, l)

            @pl.when(lax.rem(j, 2) == 0)
            def _():
                sums(q0 + i)

            @pl.when(lax.rem(j, 2) == 1)
            def _():
                emit(q0 + i)
                if l == 0:

                    @pl.when(i == 0)
                    def _():
                        on_chip(CH)

            return 0

        if l == 1:
            arrive(CH)
        for h in range(2):
            first_half(0, 0, l, h)
        lax.fori_loop(0, PAIRS - 1, pair, 0)
        both(2 * PAIRS - 2, 0, l)
        second(2 * PAIRS - 1, 1, l)
        emit(q0 + CH - 1)

    layer_back(1)

    def norm_back(rows):
        h, da = H[rows, :].astype(F32), ACC[rows, :].astype(BF16).astype(F32)
        scale = lax.rsqrt(jnp.mean(h * h, -1, keepdims=True) + 1e-6)
        inner = jnp.sum(da * h, -1, keepdims=True)
        by_h = da * scale - h * (inner * scale * scale * scale * (1.0 / D))
        DY[rows, :] = (DY[rows, :].astype(F32) + by_h.astype(BF16).astype(F32)).astype(BF16)

    tiles(norm_back)
    on_chip(CH - 1)
    transposed(DY, DYT)

    layer_back(0)

    on_chip(N - 1)
    for q in range(N - 4, N):
        final(q)

    S[0] = SQ[:, 0:128] + SQ[:, 128:256] + SQ[:, 256:384] + SQ[:, 384:512]
    put_wait(0)
    put_wait(1)

    def drain(u, _):
        move_x(u).wait_send()
        move_y(u, half).wait_send()
        move_e(u, xp).wait_send()
        return 0

    lax.fori_loop(0, 3 * N, drain, 0)

    def share(k, to):
        move = remote(S.at[k], SR.at[k], ss.at[k], sr.at[k], to)
        move.start()
        move.wait()

    share(0, to_mate)
    S[1] = S[0] + SR[0]

    def drain_d(n, _):
        move_d(n, me).wait_send()
        return 0

    lax.fori_loop(0, N, drain_d, 0)
    for q in range(N - 2, N):
        to_core(q).wait_send()
    for q in range(N - 3, N):
        to_chip(q).wait_send()
    share(1, to_x)
    sq_ref[...] = S[1] + SR[1]


def gradients(x, dy, wg, wu, wd):
    any_space, vmem = pl.BlockSpec(memory_space=pl.ANY), pl.BlockSpec(memory_space=pltpu.VMEM)
    sem = pltpu.SemaphoreType.DMA
    sems = [sem((3 * N,))] * 6 + [sem((N,))] * 7 + [sem((3,)), sem((2,)), sem((2,)), sem((2,)), pltpu.SemaphoreType.REGULAR]
    block = (3, B, 512)
    return pl.pallas_call(
        kernel,
        out_shape=(
            jax.ShapeDtypeStruct(wg.shape, BF16),
            jax.ShapeDtypeStruct(wu.shape, BF16),
            jax.ShapeDtypeStruct(wd.shape, BF16),
            jax.ShapeDtypeStruct((8, 128), F32),
        ),
        in_specs=[any_space] * 5,
        out_specs=(any_space, any_space, any_space, vmem),
        scratch_shapes=[
            pltpu.VMEM((2, CH, 4) + block, BF16),
            pltpu.VMEM((T, D), BF16),
            pltpu.VMEM((D, T), BF16),
            pltpu.VMEM((T, D), BF16),
            pltpu.VMEM((D, T), BF16),
            pltpu.VMEM((T, D), BF16),
            pltpu.VMEM((T, D), BF16),
            pltpu.VMEM((D, T), BF16),
            pltpu.VMEM((T, D), F32),
        ]
        + [pltpu.VMEM((TT, C), BF16)] * 6
        + [
            pltpu.VMEM((3, 512, 512), F32),
            pltpu.VMEM((2, 2, 2) + block, BF16),
            pltpu.VMEM((2, 2) + block, BF16),
            pltpu.VMEM((3,) + block, BF16),
            pltpu.VMEM((6,) + block, BF16),
            pltpu.VMEM((4,) + block, F32),
            pltpu.VMEM((2,) + block, BF16),
            pltpu.VMEM((8, 512), F32),
            pltpu.VMEM((2, 8, 128), F32),
            pltpu.VMEM((2, 8, 128), F32),
        ]
        + sems,
        compiler_params=pltpu.CompilerParams(collective_id=0, has_side_effects=True, vmem_limit_bytes=67043328),
        name="step",
    )(x, dy, wg, wu, wd)


def adamw(w, m, v, g):
    m = 0.9 * m + 0.1 * g
    v = 0.95 * v + 0.05 * g * g
    step = m * lax.rsqrt(v + 1e-8) + 0.1 * w
    return (w - 0.02 * step).astype(BF16), m, v


def solution(mesh):
    def step(x, dy, *arrays):
        weights, m, v = (arrays[i : i + 3] for i in (0, 3, 6))
        *grads, squares = gradients(x[0], dy[0], *weights)
        total = jnp.sum(squares)
        count = 4 * sum(g.size for g in grads)
        factor = jnp.minimum(1.0, 0.5 * lax.rsqrt(total / count + 1e-30))
        new = [adamw(w.astype(F32), m, v, g.astype(F32) * factor) for w, m, v, g in zip(weights, m, v, grads, strict=True)]
        return tuple(one[which] for which in range(3) for one in new)

    states, cut = P(("rep", "dp"), None, None), P(None, "dp", None)
    return jax.shard_map(
        step,
        mesh=mesh,
        in_specs=(states, states) + (cut,) * 9,
        out_specs=(P("rep", "dp", None),) * 9,
        check_vma=False,
    )
```

```python
import functools

import jax
import jax.numpy as jnp
from jax import lax
from jax.experimental import pallas as pl
from jax.experimental.pallas import tpu as pltpu
from jax.sharding import PartitionSpec as P

MESH = pl.DeviceIdType.MESH
F32, BF16 = jnp.float32, jnp.bfloat16
T, D, FF = 2048, 512, 4096
CH = 8
B = 128
C = 4 * B
TT = 512
N = 2 * CH


def dot(a, b):
    return jnp.dot(a, b, preferred_element_type=F32)


def dot_nt(a, b):
    return lax.dot_general(a, b, (((1,), (1,)), ((), ())), preferred_element_type=F32)


def normed(h):
    wide = h.astype(F32)
    return (wide * lax.rsqrt(jnp.mean(wide * wide, -1, keepdims=True) + 1e-6)).astype(BF16)


def kernel(
    x_ref, dy_ref, wg_ref, wu_ref, wd_ref, gg_ref, gu_ref, gd_ref, sq_ref,
    W, A0, A0T, A1, A1T, H, DY, DYT, ACC, PB0, PB1, DG0, DG1, DU0, DU1, AW, G, R, X, XR, SO, GB, SQ, S, SR,
    xs, xr, ys, yr, es, er, own_s, ds, dr, rs, rr, zs, zr, ld, gs, ss, sr, credit,
):
    me, rep = lax.axis_index("dp"), lax.axis_index("rep")
    core, chip = lax.rem(me, 2), lax.div(me, 2)
    xp, mate = lax.rem(me + 2, 4), me + 1 - 2 * core
    matexp = lax.rem(mate + 2, 4)
    to_x, to_mate, to_y = {"dp": xp}, {"dp": mate}, {"rep": 1 - rep}
    half = pl.ds(pl.multiple_of(64 * rep, 64), 64)
    other_half = pl.ds(pl.multiple_of(64 * (1 - rep), 64), 64)

    barrier = pltpu.get_barrier_semaphore()
    for to in (to_x, to_mate, to_y):
        pl.semaphore_signal(barrier, inc=1, device_id=to, device_id_type=MESH)

    def split(n):
        return lax.div(n, CH), lax.rem(n, CH)

    def own(n, _):
        l, i = split(n)
        for d in range(4):
            cols = pl.ds(pl.multiple_of(1024 * d + B * i, B), B)
            pltpu.make_async_copy(wg_ref.at[l, :, cols], W.at[l, i, me, 0, :, pl.ds(B * d, B)], own_s.at[n]).start()
            pltpu.make_async_copy(wu_ref.at[l, :, cols], W.at[l, i, me, 1, :, pl.ds(B * d, B)], own_s.at[n]).start()
        pltpu.make_async_copy(wd_ref.at[l, pl.ds(pl.multiple_of(B * i, B), B), :], W.at[l, i, me, 2], own_s.at[n]).start()
        return 0

    lax.fori_loop(0, CH, own, 0)
    pltpu.make_async_copy(x_ref, A0, ld.at[0]).start()
    pltpu.make_async_copy(dy_ref, DY, ld.at[1]).start()
    pltpu.make_async_copy(x_ref, H, ld.at[2]).start()
    lax.fori_loop(CH, N, own, 0)

    def remote(src, dst, s, r, to):
        return pltpu.make_async_remote_copy(src_ref=src, dst_ref=dst, send_sem=s, recv_sem=r, device_id=to, device_id_type=MESH)

    def piece(u):
        n = lax.div(u, 3)
        return split(n) + (lax.rem(u, 3),)

    def move_x(u, block=None):
        l, i, j = piece(u)
        ref = W.at[l, i, me if block is None else block, j, half, :]
        return remote(ref, ref, xs.at[u], xr.at[u], to_x)

    def move_y(u, which):
        l, i, j = piece(u)
        ref = W.at[l, i, xp, j, which, :]
        return remote(ref, ref, ys.at[u], yr.at[u], to_y)

    def move_e(u, block):
        l, i, j = piece(u)
        ref = W.at[l, i, block, j]
        return remote(ref, ref, es.at[u], er.at[u], to_mate)

    def move_d(n, block):
        l, i = split(n)
        ref = W.at[l, i, block]
        return remote(ref, ref, ds.at[n], dr.at[n], to_mate)

    pl.semaphore_wait(barrier, 3)

    def send_own(n, _):
        l, i = split(n)
        pltpu.make_async_copy(W.at[l, i, me], W.at[l, i, me], own_s.at[n]).wait()
        for j in range(3):
            move_x(3 * n + j).start()
        move_d(n, me).start()
        return 0

    lax.fori_loop(0, N, send_own, 0)

    def pump_x(u):
        move_x(u, xp).wait_recv()
        move_y(u, half).start()

    def pump_y(u):
        move_y(u, other_half).wait_recv()
        move_e(u, xp).start()

    def arrive(n):
        move_d(n, mate).wait_recv()
        for j in range(3):
            move_e(3 * n + j, matexp).wait_recv()

    def tiles(body):
        def one(t, _):
            body(pl.ds(pl.multiple_of(t * TT, TT), TT))
            return 0

        lax.fori_loop(0, T // TT, one, 0)

    def columns(t):
        return pl.ds(pl.multiple_of(t * TT, TT), TT)

    def transposed(src, dst):
        def one(t, _):
            dst[:, columns(t)] = src[columns(t), :].T
            return 0

        lax.fori_loop(0, T // TT, one, 0)

    pltpu.make_async_copy(x_ref, A0, ld.at[0]).wait()

    def norm_a(rows):
        A0[rows, :] = normed(A0[rows, :])
        ACC[rows, :] = jnp.zeros((TT, D), F32)

    tiles(norm_a)
    pump_x(0)
    pump_x(1)
    pltpu.make_async_copy(dy_ref, DY, ld.at[1]).wait()
    transposed(DY, DYT)
    pump_x(2)
    pump_y(0)
    pltpu.make_async_copy(x_ref, H, ld.at[2]).wait()
    transposed(A0, A0T)
    SQ[...] = jnp.zeros_like(SQ)
    pump_x(3)
    pump_y(1)
    pump_x(4)
    pump_y(2)

    def matrix(l, i, which):
        return W[l, i, :, which].reshape(4 * B, 512)

    def forward(i, _):
        arrive(i)
        for t in range(T // TT):
            if t != 1:
                pump_x(3 * i + 5 + max(t - 1, 0))
            if t > 0:
                pump_y(3 * i + 2 + t)
            rows = slice(t * TT, (t + 1) * TT)
            a = A0[rows, :]
            gate, up = dot(a, matrix(0, i, 0)), dot(a, matrix(0, i, 1))
            p = (gate * jax.nn.sigmoid(gate) * up).astype(BF16)
            ACC[rows, :] += dot(p, matrix(0, i, 2))
        return 0

    lax.fori_loop(0, CH, forward, 0)

    def between(rows):
        h = (H[rows, :].astype(F32) + ACC[rows, :].astype(BF16).astype(F32)).astype(BF16)
        H[rows, :] = h
        A1[rows, :] = normed(h)
        ACC[rows, :] = jnp.zeros((TT, D), F32)

    tiles(between)
    transposed(A1, A1T)

    def to_core(q):
        return remote(G.at[lax.rem(q, 2), 1 - core], R.at[lax.rem(q, 2)], rs.at[q], rr.at[q], to_mate)

    def to_chip(q):
        return remote(X.at[lax.rem(q, 3)], XR.at[lax.rem(q, 6)], zs.at[q], zr.at[q], to_x)

    def on_chip(q):
        slot = lax.rem(q, 2)
        to_core(q).wait_recv()

        @pl.when(q >= 3)
        def _():
            to_chip(q - 3).wait_send()

        for j in range(3):
            X[lax.rem(q, 3), j] = (G[slot, core, 1 - chip, j].astype(F32) + R[slot, 1 - chip, j].astype(F32)).astype(BF16)
            SO[lax.rem(q, 4), j] = G[slot, core, chip, j].astype(F32) + R[slot, chip, j].astype(F32)

        @pl.when(q >= 6)
        def _():
            pl.semaphore_wait(credit, 1)

        to_chip(q).start()

    def put(q, slot):
        l, i = 1 - lax.div(q, CH), lax.rem(q, CH)
        for d in range(4):
            cols = pl.ds(pl.multiple_of(1024 * d + B * i, B), B)
            pltpu.make_async_copy(GB.at[slot, 0, :, pl.ds(B * d, B)], gg_ref.at[l, :, cols], gs.at[slot]).start()
            pltpu.make_async_copy(GB.at[slot, 1, :, pl.ds(B * d, B)], gu_ref.at[l, :, cols], gs.at[slot]).start()
        pltpu.make_async_copy(GB.at[slot, 2], gd_ref.at[l, pl.ds(pl.multiple_of(B * i, B), B), :], gs.at[slot]).start()

    def put_wait(slot):
        pltpu.make_async_copy(GB.at[slot], GB.at[slot], gs.at[slot]).wait()

    def final(q):
        slot = lax.rem(q, 2)
        to_chip(q).wait_recv()

        @pl.when(q >= 2)
        def _():
            put_wait(slot)

        for j in range(3):
            g = (SO[lax.rem(q, 4), j] + XR[lax.rem(q, 6), j].astype(F32)).astype(BF16)
            GB[slot, j] = g
            wide = g.astype(F32)
            SQ[...] += jnp.sum((wide * wide).reshape(B // 8, 8, 512), axis=0)

        @pl.when(q < N - 6)
        def _():
            pl.semaphore_signal(credit, inc=1, device_id=to_x, device_id_type=MESH)

        put(q, slot)

    PB, DG, DU = (PB0, PB1), (DG0, DG1), (DU0, DU1)

    def tokens(n):
        return pl.ds(pl.multiple_of(lax.rem(n, 4) * TT, TT), TT)

    def first_half(n, slot, l, h):
        i, rows, cols = lax.div(n, 4), tokens(n), slice(256 * h, 256 * (h + 1))
        a, by = (A0, A1)[l][rows, :], DY[rows, :]
        gate = dot(a, W[l, i, :, 0, :, cols].reshape(D, 256))
        up = dot(a, W[l, i, :, 1, :, cols].reshape(D, 256))
        dp = dot_nt(by, W[l, i, 2 * h : 2 * h + 2, 2].reshape(256, D)).astype(BF16).astype(F32)
        s = jax.nn.sigmoid(gate)
        silu = gate * s
        PB[slot][:, cols] = (silu * up).astype(BF16)
        DU[slot][:, cols] = (dp * silu).astype(BF16)
        DG[slot][:, cols] = (dp * up * (s + silu * (1.0 - s))).astype(BF16)

    def by_input(n, slot, l):
        if l == 1:
            i, rows = lax.div(n, 4), tokens(n)
            ACC[rows, :] += dot_nt(DG[slot][...], matrix(l, i, 0)) + dot_nt(DU[slot][...], matrix(l, i, 1))

    def by_weight(n, slot, l, j):
        left = (A0T, A1T)[l] if j < 2 else DYT
        right = (DG, DU, PB)[j][slot]
        new = dot(left[:, tokens(n)], right[...])
        AW[j] = jnp.where(lax.rem(n, 4) == 0, 0.0, AW[j]) + new

    def both(n, slot, l):
        first_half(n + 1, 1 - slot, l, 0)
        by_input(n, slot, l)
        if l == 0:
            by_weight(n, slot, l, 0)
        first_half(n + 1, 1 - slot, l, 1)
        for j in range(1 - l, 3):
            by_weight(n, slot, l, j)

    def second(n, slot, l):
        by_input(n, slot, l)
        for j in range(3):
            by_weight(n, slot, l, j)

    def emit(q):
        @pl.when(q >= 2)
        def _():
            to_core(q - 2).wait_send()

        slot = lax.rem(q, 2)
        for j in range(3):
            by_w = AW[j].T.astype(BF16) if j == 2 else AW[j].astype(BF16)
            for d in range(4):
                G[slot, d % 2, d // 2, j] = by_w[B * d : B * (d + 1)]
        to_core(q).start()

    def sums(q):
        @pl.when(q >= 4)
        def _():
            final(q - 4)

        @pl.when((q >= 1) & (q != CH))
        def _():
            on_chip(q - 1)

    PAIRS = 2 * CH

    def layer_back(l):
        q0 = CH * (1 - l)

        def pair(j, _):
            i = lax.div(j, 2)
            if l == 1:
                for k in range(3):

                    @pl.when((26 + 3 * j + k >= 27) & (26 + 3 * j + k < 3 * N))
                    def _():
                        pump_y(26 + 3 * j + k)

                for k in range(3):

                    @pl.when(29 + 3 * j + k < 3 * N)
                    def _():
                        pump_x(29 + 3 * j + k)

                @pl.when(lax.rem(j, 2) == 1)
                def _():
                    arrive(CH + i + 1)

            both(2 * j, 0, l)

            @pl.when(lax.rem(j, 2) == 0)
            def _():
                sums(q0 + i)

            both(2 * j + 1, 1, l)

            @pl.when(lax.rem(j, 2) == 1)
            def _():
                emit(q0 + i)

            return 0

        if l == 1:
            arrive(CH)
        for h in range(2):
            first_half(0, 0, l, h)
        lax.fori_loop(0, PAIRS - 1, pair, 0)
        both(2 * PAIRS - 2, 0, l)
        second(2 * PAIRS - 1, 1, l)
        emit(q0 + CH - 1)

    layer_back(1)

    def norm_back(rows):
        h, da = H[rows, :].astype(F32), ACC[rows, :].astype(BF16).astype(F32)
        scale = lax.rsqrt(jnp.mean(h * h, -1, keepdims=True) + 1e-6)
        inner = jnp.sum(da * h, -1, keepdims=True)
        by_h = da * scale - h * (inner * scale * scale * scale * (1.0 / D))
        DY[rows, :] = (DY[rows, :].astype(F32) + by_h.astype(BF16).astype(F32)).astype(BF16)

    tiles(norm_back)
    on_chip(CH - 1)
    transposed(DY, DYT)

    layer_back(0)

    on_chip(N - 1)
    for q in range(N - 4, N):
        final(q)

    S[0] = SQ[:, 0:128] + SQ[:, 128:256] + SQ[:, 256:384] + SQ[:, 384:512]
    put_wait(0)
    put_wait(1)

    def drain(u, _):
        move_x(u).wait_send()
        move_y(u, half).wait_send()
        move_e(u, xp).wait_send()
        return 0

    lax.fori_loop(0, 3 * N, drain, 0)

    def share(k, to):
        move = remote(S.at[k], SR.at[k], ss.at[k], sr.at[k], to)
        move.start()
        move.wait()

    share(0, to_mate)
    S[1] = S[0] + SR[0]

    def drain_d(n, _):
        move_d(n, me).wait_send()
        return 0

    lax.fori_loop(0, N, drain_d, 0)
    for q in range(N - 2, N):
        to_core(q).wait_send()
    for q in range(N - 3, N):
        to_chip(q).wait_send()
    share(1, to_x)
    sq_ref[...] = S[1] + SR[1]


def gradients(x, dy, wg, wu, wd):
    any_space, vmem = pl.BlockSpec(memory_space=pl.ANY), pl.BlockSpec(memory_space=pltpu.VMEM)
    sem = pltpu.SemaphoreType.DMA
    sems = [sem((3 * N,))] * 6 + [sem((N,))] * 7 + [sem((3,)), sem((2,)), sem((2,)), sem((2,)), pltpu.SemaphoreType.REGULAR]
    block = (3, B, 512)
    return pl.pallas_call(
        kernel,
        out_shape=(
            jax.ShapeDtypeStruct(wg.shape, BF16),
            jax.ShapeDtypeStruct(wu.shape, BF16),
            jax.ShapeDtypeStruct(wd.shape, BF16),
            jax.ShapeDtypeStruct((8, 128), F32),
        ),
        in_specs=[any_space] * 5,
        out_specs=(any_space, any_space, any_space, vmem),
        scratch_shapes=[
            pltpu.VMEM((2, CH, 4) + block, BF16),
            pltpu.VMEM((T, D), BF16),
            pltpu.VMEM((D, T), BF16),
            pltpu.VMEM((T, D), BF16),
            pltpu.VMEM((D, T), BF16),
            pltpu.VMEM((T, D), BF16),
            pltpu.VMEM((T, D), BF16),
            pltpu.VMEM((D, T), BF16),
            pltpu.VMEM((T, D), F32),
        ]
        + [pltpu.VMEM((TT, C), BF16)] * 6
        + [
            pltpu.VMEM((3, 512, 512), F32),
            pltpu.VMEM((2, 2, 2) + block, BF16),
            pltpu.VMEM((2, 2) + block, BF16),
            pltpu.VMEM((3,) + block, BF16),
            pltpu.VMEM((6,) + block, BF16),
            pltpu.VMEM((4,) + block, F32),
            pltpu.VMEM((2,) + block, BF16),
            pltpu.VMEM((8, 512), F32),
            pltpu.VMEM((2, 8, 128), F32),
            pltpu.VMEM((2, 8, 128), F32),
        ]
        + sems,
        compiler_params=pltpu.CompilerParams(collective_id=0, has_side_effects=True, vmem_limit_bytes=67043328),
        name="step",
    )(x, dy, wg, wu, wd)


def adamw(w, m, v, g):
    m = 0.9 * m + 0.1 * g
    v = 0.95 * v + 0.05 * g * g
    step = m * lax.rsqrt(v + 1e-8) + 0.1 * w
    return (w - 0.02 * step).astype(BF16), m, v


def solution(mesh):
    def step(x, dy, *arrays):
        weights, m, v = (arrays[i : i + 3] for i in (0, 3, 6))
        *grads, squares = gradients(x[0], dy[0], *weights)
        total = jnp.sum(squares)
        count = 4 * sum(g.size for g in grads)
        factor = jnp.minimum(1.0, 0.5 * lax.rsqrt(total / count + 1e-30))
        new = [adamw(w.astype(F32), m, v, g.astype(F32) * factor) for w, m, v, g in zip(weights, m, v, grads, strict=True)]
        return tuple(one[which] for which in range(3) for one in new)

    states, cut = P(("rep", "dp"), None, None), P(None, "dp", None)
    return jax.shard_map(
        step,
        mesh=mesh,
        in_specs=(states, states) + (cut,) * 9,
        out_specs=(P("rep", "dp", None),) * 9,
        check_vma=False,
    )
```
